32 devices in a mesh: dp: 4 (over z), expert: 4 (over y, x), tensor: 2 (over core).
Axes of the slice: x: 2, y: 2, z: 4, core: 2. Of those that a mesh axis runs over, the one named last changes fastest.
Arguments:
- tokens: bfloat16 [192, 7168], P(('dp', 'expert')), may hold values from -6 to 6
- expert_ids: int32 [192, 8], P(('dp', 'expert')), may hold values from 0 to 15, all different within a row; in each aligned block of 12 rows (0 to 11, 12 to 23, ...) at most 8 rows name the same one
- route_weights: float32 [192, 8], P(('dp', 'expert')), may hold values from 0.1 to 1
- gate_weights: bfloat16 [16, 7168, 2048], P('expert', 'dp', 'tensor'), may hold values from -0.0625 to 0.0625
- up_weights: bfloat16 [16, 7168, 2048], P('expert', 'dp', 'tensor'), may hold values from -0.0625 to 0.0625
- down_weights: bfloat16 [16, 2048, 7168], P('expert', 'tensor', 'dp'), may hold values from -0.125 to 0.125
- shared_gate: bfloat16 [7168, 2048], P('dp', 'tensor'), may hold values from -0.0625 to 0.0625
- shared_up: bfloat16 [7168, 2048], P('dp', 'tensor'), may hold values from -0.0625 to 0.0625
- shared_down: bfloat16 [2048, 7168], P('tensor', 'dp'), may hold values from -0.125 to 0.125
Outputs:
- mixed: bfloat16 [192, 7168], P(('dp', 'expert'))
The draws below stay inside these ranges and needn't reach their ends.
Inputs may be any that keep to these rules, and one draw needn't show every extreme that they name: `expert_ids`: each token names 8 different experts. In the rows of one device no expert is named by more than 8 tokens, and in some device's rows some expert is named by exactly 8.
All inputs are finite; a program needn't handle non-finite values.
Results may differ from the reference program's by a relative error of at most 0.005.
Values may be sent and summed in bfloat16 or wider, within the bound.
A program may use at most 128 MiB of HBM per device.

```python
import math
import jax
import jax.numpy as jnp
import numpy as np
from jax import lax

D = 7168
FF = 2048
TOP = 8
EXPERTS = 16
TOK_DEV = 12
CAP = 8
TOKENS = 192


def block_levels(own_key, shape, shards, smallest, high):
    gain, own = 1.0, jax.random.fold_in(own_key, 6)
    for axis_at, shards_of in shards:
        heights = jnp.exp(jax.random.uniform(jax.random.fold_in(own, axis_at), (shards_of,), jnp.float32, smallest / len(shards), high / len(shards)))
        gain = gain * jnp.repeat(heights, shape[axis_at] // shards_of).reshape([-1 if axis == axis_at else 1 for axis in range(len(shape))])
    return gain


def assign_block(stream_key, own, number, rows, amount, top, limit, skew):
    sequence = jax.random.permutation(stream_key, amount)
    packed, common = shares(amount, rows * top, limit, skew, True), shares(amount, rows * top, limit, skew, False)
    places = jnp.arange(amount)

    def named(lengths, offset_by):
        used = int((lengths > 0).sum())
        fixed = max(1, used // 4)
        passed = fixed + (places - fixed + offset_by * (used - fixed)) % max(1, amount - fixed)
        return jnp.zeros((amount,), jnp.int32).at[sequence[jnp.where(places < fixed, places, passed)]].set(jnp.asarray(lengths, jnp.int32))

    lengths = jnp.where(number % 4 == 0, named(packed, number // 4), named(common, number - number // 4 - 1))
    mixed = jax.random.permutation(jax.random.fold_in(own, 3), amount)
    donor, sink = mixed[0:amount // 2 * 2:2], mixed[1:amount // 2 * 2:2]
    margin = jnp.minimum(lengths[donor] - 1, limit - lengths[sink]) // 2
    margin = jnp.where((donor == sequence[0]) | (sink == sequence[0]) | (lengths[sink] == 0), 0, jnp.maximum(margin, 0))
    passed = jax.random.randint(jax.random.fold_in(own, 4), (amount // 2,), 0, 1 << 20) % (margin + 1)
    lengths = lengths.at[donor].add(-passed).at[sink].add(passed)
    labels = jnp.searchsorted(jnp.cumsum(lengths), jnp.arange(rows * top), side="right").astype(jnp.int32)
    table = labels.reshape(top, rows).T
    table = table[jax.random.permutation(jax.random.fold_in(own, 1), rows)]
    offset_by = jax.random.randint(jax.random.fold_in(own, 2), (rows, 1), 0, top)
    return jnp.take_along_axis(table, (jnp.arange(top)[None, :] + offset_by) % top, axis=1)


def shares(number_of, total, limit, lean, full):
    loads = [(1 << 20) // math.isqrt(grade ** lean) + 1 for grade in range(1, number_of + 1)]
    largest = limit if full else min(limit, max(-(-total // number_of), total * loads[0] // sum(loads)))
    least = 1 if total - largest >= number_of - 1 else 0
    counts, spare = [largest] + [least] * (number_of - 1), total - largest - least * (number_of - 1)
    while spare > 0:
        movable = [i for i in range(1, number_of) if counts[i] < largest] or [i for i in range(1, number_of) if counts[i] < limit]
        mass, remaining = sum([loads[i] for i in movable]), spare
        for i in movable:
            addition = min(limit - counts[i], max(1, remaining * loads[i] // mass), spare)
            counts[i] = counts[i] + addition
            spare = spare - addition
    return np.array(counts)


def noise(key, shape, width, limit, cuts=(), kind=jnp.bfloat16):
    gain = block_levels(key, shape, cuts, -0.22, 0.18) if cuts else 1.0
    array = jax.random.normal(key, shape, jnp.float32) * width * gain
    return jnp.minimum(jnp.maximum(array, -limit), limit).astype(kind)


def setup_inputs(seed: int = 0) -> dict:
    key_of = jax.random.split(jax.random.key(seed), 10)
    tokens = noise(key_of[0], (TOKENS, D), 1.0, 6.0, ((0, 16),))
    expert_ids_keys = jax.random.split(jax.random.fold_in(key_of[1], 1), TOKENS // TOK_DEV)
    expert_ids_turns = jax.random.permutation(jax.random.fold_in(key_of[1], 3), TOKENS // TOK_DEV)
    expert_ids = jax.vmap(lambda own, number: assign_block(jax.random.fold_in(key_of[1], 2), own, number, TOK_DEV, EXPERTS, TOP, CAP, 2))(expert_ids_keys, expert_ids_turns).reshape((TOKENS, TOP))
    route_weights = jnp.clip(jnp.exp(math.log(1.0) - 2.3025851 * jax.random.uniform(key_of[2], (TOKENS, TOP), jnp.float32) ** block_levels(key_of[2], (TOKENS, TOP), ((0, 16),), -0.2, 0.2)), 0.1, 1.0)
    gate_weights = noise(key_of[3], (EXPERTS, D, FF), D ** -0.5, 0.0625, ((0, 4), (1, 4), (2, 2)))
    up_weights = noise(key_of[4], (EXPERTS, D, FF), D ** -0.5, 0.0625, ((0, 4), (1, 4), (2, 2)))
    down_weights = noise(key_of[5], (EXPERTS, FF, D), FF ** -0.5, 0.125, ((0, 4), (1, 2), (2, 4)))
    shared_gate = noise(key_of[6], (D, FF), D ** -0.5, 0.0625, ((0, 4), (1, 2)))
    shared_up = noise(key_of[7], (D, FF), D ** -0.5, 0.0625, ((0, 4), (1, 2)))
    shared_down = noise(key_of[8], (FF, D), FF ** -0.5, 0.125, ((0, 2), (1, 4)))
    return dict(tokens=tokens, expert_ids=expert_ids, route_weights=route_weights, gate_weights=gate_weights, up_weights=up_weights, down_weights=down_weights, shared_gate=shared_gate, shared_up=shared_up, shared_down=shared_down)


def reference(tokens, expert_ids, route_weights, gate_weights, up_weights, down_weights, shared_gate, shared_up, shared_down):
    shared_gate_out = jnp.dot(tokens, shared_gate, preferred_element_type=jnp.float32)
    shared_up_out = jnp.dot(tokens, shared_up, preferred_element_type=jnp.float32)
    shared_hidden = (jax.nn.silu(shared_gate_out) * shared_up_out).astype(jnp.bfloat16)
    shared_out = jnp.dot(shared_hidden, shared_down, preferred_element_type=jnp.float32)

    def accumulate(running, layer_pack):
        gate_matrix, up_matrix, down_matrix, expert_index = layer_pack
        gate_out = jnp.dot(tokens, gate_matrix, preferred_element_type=jnp.float32)
        up_out = jnp.dot(tokens, up_matrix, preferred_element_type=jnp.float32)
        hidden = (jax.nn.silu(gate_out) * up_out).astype(jnp.bfloat16)
        expert_out = jnp.dot(hidden, down_matrix, preferred_element_type=jnp.float32)
        coefficient = jnp.sum(jnp.where(expert_ids == expert_index, route_weights, jnp.zeros_like(route_weights)), axis=1)
        return running + coefficient[:, None] * expert_out.astype(running.dtype), None

    indices = jnp.arange(EXPERTS, dtype=jnp.int32)
    running, unused = lax.scan(accumulate, shared_out, (gate_weights, up_weights, down_weights, indices))
    return running.astype(jnp.bfloat16)
```

```python
import functools

import jax
import jax.numpy as jnp
from jax import lax
from jax.experimental import pallas as pl
from jax.experimental.pallas import tpu as pltpu
from jax.sharding import PartitionSpec as P

CAP = 8
STEPS = 8
MESH = pl.DeviceIdType.MESH
VMEM = pl.BlockSpec(memory_space=pltpu.VMEM)
DMA = pltpu.SemaphoreType.DMA


def greet(peers):
    barrier = pltpu.get_barrier_semaphore()
    for peer in peers:
        pl.semaphore_signal(barrier, inc=1, device_id=peer, device_id_type=MESH)
    pl.semaphore_wait(barrier, len(peers))


def remote(src, dst, send, recv, peer):
    return pltpu.make_async_remote_copy(
        src_ref=src, dst_ref=dst, send_sem=send, recv_sem=recv, device_id=peer, device_id_type=MESH
    )


def params(number):
    return pltpu.CompilerParams(
        collective_id=number, has_side_effects=True, vmem_limit_bytes=60 * 1024 * 1024
    )


def squared(v):
    return v * jnp.abs(v)


def rooted(v):
    v = v.astype(jnp.float32)
    root = jnp.sqrt(jnp.abs(v))
    return jnp.where(v < 0.0, -root, root)


def dispatch_kernel(n, g, tok, coef, x, w, own, s1, r1, s2, r2):
    d, e = lax.axis_index("dp"), lax.axis_index("expert")
    greet(
        [{"dp": lax.rem(d + k, n)} for k in range(1, n)]
        + [{"expert": lax.rem(e + j, g)} for j in range(1, g)]
    )
    mine = [
        pltpu.make_async_copy(tok.at[d], x.at[d, e], own.at[0]),
        pltpu.make_async_copy(coef, w.at[d, e], own.at[1]),
    ]
    for copy in mine:
        copy.start()
    sends = []
    for k in range(1, n):
        to = lax.rem(d + k, n)
        for src, dst, a in ((tok.at[to], x.at[d, e], 0), (coef, w.at[d, e], 1)):
            copy = remote(src, dst, s1.at[a, k], r1.at[a, k], {"dp": to})
            copy.start()
            sends.append(copy)
    for k in range(n):
        block = lax.rem(d - k + n, n)
        for a, ref in ((0, x), (1, w)):
            if k == 0:
                mine[a].wait()
            else:
                remote(ref.at[block, e], ref.at[block, e], s1.at[a, k], r1.at[a, k], {"dp": d}).wait_recv()
            for j in range(1, g):
                copy = remote(
                    ref.at[block, e], ref.at[block, e], s2.at[a, k, j], r2.at[a, k, j],
                    {"expert": lax.rem(e + j, g)},
                )
                copy.start()
                sends.append(copy)
    for k in range(n):
        block = lax.rem(d - k + n, n)
        for a, ref in ((0, x), (1, w)):
            for j in range(1, g):
                at = ref.at[block, lax.rem(e - j + g, g)]
                remote(at, at, s2.at[a, k, j], r2.at[a, k, j], {"expert": e}).wait_recv()
    for copy in sends:
        copy.wait_send()


def dispatch(blocks, coef, n, g):
    return pl.pallas_call(
        functools.partial(dispatch_kernel, n, g),
        out_shape=(
            jax.ShapeDtypeStruct((n, g) + blocks.shape[1:], blocks.dtype),
            jax.ShapeDtypeStruct((n, g) + coef.shape, coef.dtype),
        ),
        in_specs=[VMEM] * 2,
        out_specs=(VMEM, VMEM),
        scratch_shapes=[
            DMA((2,)), DMA((2, n)), DMA((2, n)), DMA((2, n, g)), DMA((2, n, g)),
        ],
        compiler_params=params(0),
    )(blocks, coef)


def chain_kernel(
    n, steps, gate, up, scale, sgate, sup, hid, shid,
    got, out, sgot, sout, s1, r1, s2, r2, t1, q1, t2, q2,
):
    d = lax.axis_index("dp")
    prev, after = lax.rem(d - 1 + n, n), lax.rem(d + 1, n)
    greet([{"dp": prev}, {"dp": after}])
    place = (d, n - 1 - d)
    ahead = (jnp.minimum(d + 1, n - 1), jnp.maximum(d - 1, 0))
    behind = (jnp.maximum(d - 1, 0), jnp.minimum(d + 1, n - 1))

    routed = ((gate, up), got, out, hid, s1, r1, s2, r2)
    shared = ((sgate, sup), sgot, sout, shid, t1, q1, t2, q2)

    def partial_send(group, i, src, way):
        parts, got_, out_, hid_, sa, ra, sb, rb = group
        return [remote(src[h], got_.at[h, i], sa.at[h, i], ra.at[h, i], {"dp": ahead[way]}) for h in (0, 1)]

    def hidden_send(group, i, way):
        hid_, sb, rb = group[3], group[6], group[7]
        return remote(hid_.at[i], hid_.at[i], sb.at[i], rb.at[i], {"dp": behind[way]})

    def first(group, i, way):
        @pl.when(place[way] == 0)
        def _():
            for copy in partial_send(group, i, [part.at[i] for part in group[0]], way):
                copy.start()

    def forward(group, i, way, factor):
        parts, got_, out_, hid_ = group[:4]

        @pl.when(place[way] > 0)
        def _():
            for copy in partial_send(group, i, [got_.at[h, i] for h in (0, 1)], way):
                copy.wait_recv()
            sums = [rooted(parts[h][i]) + rooted(got_[h, i]) for h in (0, 1)]

            @pl.when(place[way] < n - 1)
            def _():
                for h in (0, 1):
                    out_[h, i] = squared(sums[h]).astype(out_.dtype)
                for copy in partial_send(group, i, [out_.at[h, i] for h in (0, 1)], way):
                    copy.start()

            @pl.when(place[way] == n - 1)
            def _():
                value = sums[0] / (1.0 + jnp.exp(-sums[0])) * sums[1]
                if factor is not None:
                    value = value * factor[i]
                hid_[i] = value.astype(hid_.dtype)
                hidden_send(group, i, way).start()

    def spread(group, i, way):
        hidden_send(group, i, way).wait_recv()

        @pl.when(place[way] > 0)
        def _():
            hidden_send(group, i, way).start()

    for s in range(steps):
        for way in (0, 1):
            first(routed, 2 * s + way, way)
    for way in (0, 1):
        first(shared, way, way)

    total = steps + 1
    for s in range(total + 2 * (n - 1)):
        for way in (0, 1):
            if s < steps:
                forward(routed, 2 * s + way, way, scale)
            elif s == steps:
                forward(shared, way, way, None)
            late = s - 2 * (n - 1 - place[way])

            @pl.when((place[way] < n - 1) & (late >= 0) & (late < steps))
            def _():
                spread(routed, 2 * late + way, way)

            @pl.when((place[way] < n - 1) & (late == steps))
            def _():
                spread(shared, way, way)

    def finish(group, i, way):
        parts, got_, out_ = group[:3]

        @pl.when(place[way] < n - 1)
        def _():
            for copy in partial_send(group, i, [out_.at[h, i] for h in (0, 1)], way):
                copy.wait_send()

        @pl.when(place[way] > 0)
        def _():
            hidden_send(group, i, way).wait_send()

    for s in range(steps):
        for way in (0, 1):
            finish(routed, 2 * s + way, way)
    for way in (0, 1):
        finish(shared, way, way)


def chain(gate, up, scale, sgate, sup, n):
    pieces, rows, width = gate.shape
    half, thin = sgate.shape[1:]
    wire = gate.dtype
    return pl.pallas_call(
        functools.partial(chain_kernel, n, pieces // 2),
        out_shape=(
            jax.ShapeDtypeStruct((pieces, rows, width), jnp.bfloat16),
            jax.ShapeDtypeStruct((2, half, thin), jnp.bfloat16),
        ),
        in_specs=[VMEM] * 5,
        out_specs=(VMEM, VMEM),
        scratch_shapes=[
            pltpu.VMEM((2, pieces, rows, width), wire),
            pltpu.VMEM((2, pieces, rows, width), wire),
            pltpu.VMEM((2, 2, half, thin), wire),
            pltpu.VMEM((2, 2, half, thin), wire),
            DMA((2, pieces)), DMA((2, pieces)), DMA((pieces,)), DMA((pieces,)),
            DMA((2, 2)), DMA((2, 2)), DMA((2,)), DMA((2,)),
        ],
        compiler_params=params(1),
    )(gate, up, scale, sgate, sup)


def collect_kernel(n, g, y, o, peer_in, z, plane, done, sa, ra, sb, rb, sc, rc, own):
    d, e, t = lax.axis_index("dp"), lax.axis_index("expert"), lax.axis_index("tensor")
    other = 1 - t
    half = n // 2
    greet(
        [{"tensor": other}]
        + [{"expert": lax.rem(e + j, g)} for j in range(1, g)]
        + [{"dp": lax.rem(d + k, n), "tensor": c} for k in range(1, n) for c in (0, 1)]
    )
    swap = []
    for j in range(g):
        to = lax.rem(e + j, g)
        copy = remote(
            y.at[pl.ds(other * half, half), to], peer_in.at[to], sa.at[j], ra.at[j], {"tensor": other}
        )
        copy.start()
        swap.append(copy)
    sends = []
    for j in list(range(1, g)) + [0]:
        to = lax.rem(e + j, g)
        swap[j].wait_recv()
        z[to] = y[pl.ds(t * half, half), to] + peer_in[to]
        if j:
            copy = remote(z.at[to], plane.at[j], sb.at[j], rb.at[j], {"expert": to})
            copy.start()
            sends.append(copy)
    total = z[e]
    for j in range(1, g):
        sends[j - 1].wait_recv()
        total = total + plane[j]
    done[...] = total.astype(done.dtype)
    last = []
    for i in range(half):
        home = t * half + i
        for c in (0, 1):
            here = (home == d) & (t == c)
            away = remote(
                done.at[i], o.at[d], sc.at[i, c], rc.at[d], {"dp": home, "tensor": c}
            )
            pl.when(jnp.logical_not(here))(away.start)
            local = pltpu.make_async_copy(done.at[i], o.at[d], own)
            pl.when(here)(local.start)
            last.append((here, away, local))
    for k in range(n):
        local_arrives = (d // half == t) & (d == k)

        @pl.when(jnp.logical_not(local_arrives))
        def _():
            remote(done.at[0], o.at[k], sc.at[0, 0], rc.at[k], {"dp": d}).wait_recv()

    for here, away, local in last:
        pl.when(jnp.logical_not(here))(away.wait_send)
        pl.when(here)(local.wait)
    for copy in swap + sends:
        copy.wait_send()


def collect(y, n, g):
    rows, width = y.shape[2:]
    half = n // 2
    return pl.pallas_call(
        functools.partial(collect_kernel, n, g),
        out_shape=jax.ShapeDtypeStruct((n, rows, width), jnp.bfloat16),
        in_specs=[VMEM],
        out_specs=VMEM,
        scratch_shapes=[
            pltpu.VMEM((g, half, rows, width), jnp.float32),
            pltpu.VMEM((g, half, rows, width), jnp.float32),
            pltpu.VMEM((g, half, rows, width), jnp.float32),
            pltpu.VMEM((half, rows, width), jnp.bfloat16),
            DMA((g,)), DMA((g,)), DMA((g,)), DMA((g,)), DMA((half, 2)), DMA((n,)), DMA,
        ],
        compiler_params=params(2),
    )(y)


def per_device(
    tokens, expert_ids, route_weights, gate_weights, up_weights, down_weights,
    shared_gate, shared_up, shared_down,
):
    g, n = lax.axis_size("expert"), lax.axis_size("dp")
    e = lax.axis_index("expert")
    rows, model = tokens.shape
    local, width, hidden = gate_weights.shape
    experts = local * g
    blocks = n * g
    count = blocks * rows
    wire = jnp.bfloat16 if n <= 4 else jnp.float32

    names = jnp.arange(experts, dtype=jnp.int32)
    coef = jnp.sum(
        jnp.where(expert_ids[:, :, None] == names, route_weights[:, :, None], 0.0), axis=1
    )
    x, w = dispatch(tokens.reshape(rows, n, width).transpose(1, 0, 2), coef, n, g)
    x = x.reshape(count, width)
    own = lax.dynamic_slice_in_dim(w.reshape(blocks, rows, experts), e * local, local, 2)
    chosen = own > 0.0
    order = jnp.tril(jnp.ones((rows, rows), jnp.float32), -1)
    place = jnp.einsum("ij,bjl->bil", order, chosen.astype(jnp.float32)).astype(jnp.int32)
    place = jnp.where(chosen, place, CAP).reshape(count, local)
    slot = jnp.arange(blocks * CAP, dtype=jnp.int32)
    block_of = jnp.arange(count, dtype=jnp.int32) // rows
    target = block_of[:, None] * CAP + place
    hit = (place < CAP).T[:, None, :] & (target.T[:, None, :] == slot[None, :, None])
    pick = hit.astype(jnp.bfloat16)
    scale = jnp.sum(jnp.where(hit, own.reshape(count, local).T[:, None, :], 0.0), axis=2)

    picked = jnp.einsum("lrt,td->lrd", pick, x, preferred_element_type=jnp.float32).astype(jnp.bfloat16)
    gate = squared(jnp.einsum("lrd,ldf->lrf", picked, gate_weights, preferred_element_type=jnp.float32)).astype(wire)
    up = squared(jnp.einsum("lrd,ldf->lrf", picked, up_weights, preferred_element_type=jnp.float32)).astype(wire)
    thin = hidden // g
    my_gate = lax.dynamic_slice_in_dim(shared_gate, e * thin, thin, 1)
    my_up = lax.dynamic_slice_in_dim(shared_up, e * thin, thin, 1)
    sgate = squared(jnp.dot(x, my_gate, preferred_element_type=jnp.float32)).astype(wire)
    sup = squared(jnp.dot(x, my_up, preferred_element_type=jnp.float32)).astype(wire)

    pieces = 2 * STEPS
    tall = local * blocks * CAP // pieces
    hid, shid = chain(
        gate.reshape(pieces, tall, hidden), up.reshape(pieces, tall, hidden),
        scale.reshape(pieces, tall, 1),
        sgate.reshape(2, count // 2, thin), sup.reshape(2, count // 2, thin), n,
    )
    hid = hid.reshape(local, blocks * CAP, hidden)
    shid = shid.reshape(count, thin)
    spread = jnp.einsum("lrt,lrf->tlf", pick, hid, preferred_element_type=jnp.float32).astype(jnp.bfloat16)
    my_down = lax.dynamic_slice_in_dim(shared_down, e * thin, thin, 0)
    y = jnp.dot(
        spread.reshape(count, local * hidden), down_weights.reshape(local * hidden, width),
        preferred_element_type=jnp.float32,
    ) + jnp.dot(shid, my_down, preferred_element_type=jnp.float32)
    o = collect(y.reshape(n, g, rows, width), n, g)
    return o.transpose(1, 0, 2).reshape(rows, model)


def solution(mesh):
    placed = (
        P(("dp", "expert"), None),
        P(("dp", "expert"), None),
        P(("dp", "expert"), None),
        P("expert", "dp", "tensor"),
        P("expert", "dp", "tensor"),
        P("expert", "tensor", "dp"),
        P("dp", "tensor"),
        P("dp", "tensor"),
        P("tensor", "dp"),
    )
    return jax.shard_map(
        per_device, mesh=mesh, in_specs=placed, out_specs=P(("dp", "expert"), None), check_vma=False
    )
```
